32 devices in a mesh: tm: 8 (over y, x, core), cell: 4 (over z).
Axes of the slice: x: 2, y: 2, z: 4, core: 2. Of those that a mesh axis runs over, the one named last changes fastest.
Arguments:
- anomalies: bfloat16 [24, 2, 8192, 256], P('tm', None, 'cell'), may hold values from -6 to 6
- obs_cells: int32 [24, 128], P('tm', 'cell'), may hold values from 0 to 8191, as said below
- obs_counts: int32 [24, 4], P('tm', 'cell'), may hold values from 16 to 32
- obs_precision: float32 [24, 128], P('tm', 'cell'), may hold values from 0.1 to 1
- inflation: float32 [24], P('tm'), may hold values from 1 to 1.12
Outputs:
- smoothed: bfloat16 [24, 2, 8192, 256], P('tm', None, 'cell')
The draws below stay inside these ranges and needn't reach their ends.
Inputs may be any that keep to these rules, and one draw needn't show every extreme that they name: `obs_cells`: slot k of a window names a cell of the block of 2048 cells that starts at (k // 32) * 2048; two slots may name the same cell.
All inputs are finite; a program needn't handle non-finite values.
Results may differ from the reference program's by a relative error of at most 0.017.
Values may be sent and summed in bfloat16 or wider, within the bound.
A program may use at most 128 MiB of HBM per device.

```python
import math
import jax
import jax.numpy as jnp
from jax import lax

M = 256
CELL_DEV = 2048
OBS_DEV = 32
WINDOWS = 24
CELLS = 8192
OBS = 128
N_CELL = 4


def draw_obs_cells(key, part):
    block = jnp.arange(OBS, dtype=jnp.int32) // OBS_DEV
    offsets = jax.random.randint(key, (WINDOWS, OBS), 0, CELL_DEV, dtype=jnp.int32)
    return offsets + block[None, :] * CELL_DEV


def set_ends(entries, rng, low, top_value):
    longest = entries.shape.index(max(entries.shape))
    spots = []
    for shift in (0, 1):
        where = [jax.random.randint(jax.random.fold_in(rng, axis), (), 0, length) for axis, length in enumerate(entries.shape)]
        where[longest] = (where[longest] + shift) % entries.shape[longest]
        spots.append(tuple(where))
    return entries.at[spots[0]].set(low).at[spots[1]].set(top_value)


def level_of(stream_key, dims, pieces, smallest, high):
    gain = 1.0
    for position, blocks in pieces:
        heights = jax.random.uniform(jax.random.fold_in(jax.random.fold_in(stream_key, 6), position), (blocks,), jnp.float32, smallest / len(pieces), high / len(pieces))
        gain = gain * jnp.repeat(jnp.exp(heights), dims[position] // blocks).reshape((-1,) + (1,) * (len(dims) - 1 - position))
    return gain


def normal_values(key, shape, deviation, reach, shards=(), kind=jnp.bfloat16):
    values = deviation * jax.random.normal(key, shape, jnp.float32)
    if shards:
        values = values * level_of(key, shape, shards, -0.22, 0.18)
    return jnp.clip(values, -reach, reach).astype(kind)


def setup_inputs(seed: int = 0) -> dict:
    streams_of = jax.random.split(jax.random.key(seed), 6)
    anomalies = normal_values(streams_of[0], (WINDOWS, 2, CELLS, M), 1.0, 6.0, ((0, 8), (2, 4)))
    obs_cells = draw_obs_cells(jax.random.fold_in(streams_of[5], 71), 0)
    obs_counts = set_ends(jax.random.randint(streams_of[2], (WINDOWS, N_CELL), OBS_DEV // 2, OBS_DEV + 1), jax.random.fold_in(streams_of[2], 1), OBS_DEV // 2, OBS_DEV).astype(jnp.int32)
    obs_precision = jnp.clip(jnp.exp(math.log(1.0) - 2.3025851 * jax.random.uniform(streams_of[3], (WINDOWS, OBS), jnp.float32) ** level_of(streams_of[3], (WINDOWS, OBS), ((0, 8), (1, 4)), -0.2, 0.2)), 0.1, 1.0)
    inflation = jnp.clip(jnp.exp(math.log(1.12) - 0.11332869 * jax.random.uniform(streams_of[4], (WINDOWS,), jnp.float32) ** level_of(streams_of[4], (WINDOWS,), ((0, 8),), -0.2, 0.2)), 1.0, 1.12)
    return {"anomalies": anomalies, "obs_cells": obs_cells, "obs_counts": obs_counts, "obs_precision": obs_precision, "inflation": inflation}


def one_transform(packed):
    field, cells, counts_row, precision, rho = packed
    picked = field[0][cells].astype(jnp.float32)
    slot = jnp.arange(OBS) % OBS_DEV
    block = jnp.arange(OBS) // OBS_DEV
    live = slot < counts_row[block]
    weights = jnp.where(live, precision, jnp.float32(0.0))
    weighted = picked * weights[:, None]
    gram = jnp.dot(weighted.T.astype(jnp.float32), picked.astype(jnp.float32), precision=lax.Precision.HIGHEST, preferred_element_type=jnp.float32)
    unit_matrix = jnp.eye(M, dtype=jnp.float32)
    system = (M - 1.0) * unit_matrix + gram
    factor = jnp.linalg.cholesky(system)
    inverse = jax.scipy.linalg.solve_triangular(factor, unit_matrix, lower=True)
    return rho * jnp.sqrt(jnp.float32(M - 1.0)) * inverse.T

def reference(anomalies, obs_cells, obs_counts, obs_precision, inflation):
    transforms = lax.map(one_transform, (anomalies, obs_cells, obs_counts, obs_precision, inflation))

    def backward(carried, current):
        product = jnp.dot(current.astype(jnp.float32), carried.astype(jnp.float32), precision=lax.Precision.HIGHEST, preferred_element_type=jnp.float32)
        return (product, product)
    unit_matrix = jnp.eye(M, dtype=jnp.float32)
    _, suffixes = lax.scan(backward, unit_matrix, transforms, reverse=True)
    weights = suffixes.astype(jnp.bfloat16)

    def apply_window(packed):
        field, weight_matrix = packed
        flat = field.reshape(2 * CELLS, M)
        result = jnp.dot(flat.astype(jnp.float32), weight_matrix.astype(jnp.float32), preferred_element_type=jnp.float32)
        return result.astype(jnp.bfloat16).reshape(2, CELLS, M)
    return lax.map(apply_window, (anomalies, weights))
```

```python
import jax
import jax.numpy as jnp
from jax import lax
from jax.experimental import pallas as pl
from jax.experimental.pallas import tpu as pltpu
from jax.sharding import PartitionSpec as P

F32 = jnp.float32
BF16 = jnp.bfloat16


def dot_any(left, right, dims):
    return lax.dot_general(left, right, (dims, ((), ())), preferred_element_type=F32)


def halves(value):
    high = value.astype(BF16)
    return high, (value - high.astype(F32)).astype(BF16)


def dot_three(left, right, dims=((1,), (0,))):
    lh, ll = halves(left)
    rh, rl = halves(right)
    return dot_any(lh, rh, dims) + (dot_any(lh, rl, dims) + dot_any(ll, rh, dims))


def dot_full(left, right, dims=((1,), (0,))):
    return lax.dot_general(
        left, right, (dims, ((), ())), precision=lax.Precision.HIGHEST, preferred_element_type=F32
    )


def eliminate(matrices):
    size = matrices[0].shape[0]
    groups = size // 8
    lane = lax.broadcasted_iota(jnp.int32, (8, size), 1)
    sub = lax.broadcasted_iota(jnp.int32, (8, size), 0)
    work = [[m[8 * g : 8 * g + 8, :] for g in range(groups)] for m in matrices]
    for k in range(size):
        g, r = divmod(k, 8)
        at_k = lane == k
        below = sub > r
        for rows in work:
            own = rows[g]
            pivot_row = jnp.broadcast_to(own[r : r + 1, :], (8, size))
            inverse = 1.0 / own[r : r + 1, k : k + 1]
            scaled = jnp.where(at_k, 1.0, pivot_row) * inverse
            for i in range(g, groups):
                column = jnp.broadcast_to(rows[i][:, k : k + 1], (8, size))
                if i == g:
                    if r == 7:
                        continue
                    column = jnp.where(below, column, 0.0)
                    base = jnp.where(at_k & below, 0.0, rows[i])
                else:
                    base = jnp.where(at_k, 0.0, rows[i])
                rows[i] = base - column * scaled
    results = []
    for rows in work:
        pieces = []
        for g in range(groups):
            row = sub + 8 * g
            pivot = jnp.sum(jnp.where(lane == row, rows[g], 0.0), axis=1, keepdims=True)
            unit = jnp.where(lane < row, rows[g], jnp.where(lane == row, 1.0, 0.0))
            pieces.append(unit * lax.rsqrt(pivot))
        results.append(jnp.concatenate(pieces, axis=0))
    return results


def transforms_kernel(
    rho_ref, picked_ref, weight_ref, partial_ref, own_ref, gram, first_inv, second_inv, low_ref, mid_ref
):
    windows = picked_ref.shape[0]
    members = picked_ref.shape[2]
    half = members // 2
    eye = (
        lax.broadcasted_iota(jnp.int32, (members, members), 0)
        == lax.broadcasted_iota(jnp.int32, (members, members), 1)
    )
    tn = ((0,), (0,))
    nt = ((1,), (1,))

    @pl.loop(0, windows)
    def _(w):
        rows = picked_ref[w]
        high, low = halves(rows.astype(F32) * weight_ref[w])
        total = dot_any(high, rows, tn) + dot_any(low, rows, tn)
        gram[w] = total + jnp.where(eye, F32(members - 1.0), 0.0)

    for w, value in enumerate(eliminate([gram[w, :half, :half] for w in range(windows)])):
        first_inv[w] = value

    @pl.loop(0, windows)
    def _(w):
        lower = dot_full(gram[w, half:, :half], first_inv[w], nt)
        low_ref[w] = lower
        gram[w, half:, half:] -= dot_full(lower, lower, nt)
        mid_ref[w] = dot_full(lower, first_inv[w])

    for w, value in enumerate(eliminate([gram[w, half:, half:] for w in range(windows)])):
        second_inv[w] = value

    zero = jnp.zeros((half, half), F32)

    @pl.loop(0, windows)
    def _(w):
        scale = rho_ref[w] * jnp.sqrt(F32(members - 1.0))
        cross = -dot_full(second_inv[w], mid_ref[w])
        partial_ref[w, :half, :half] = scale * first_inv[w].T
        partial_ref[w, :half, half:] = scale * cross.T
        partial_ref[w, half:, :half] = zero
        partial_ref[w, half:, half:] = scale * second_inv[w].T

    @pl.loop(0, windows - 1)
    def _(turn):
        w = windows - 2 - turn
        partial_ref[w] = dot_three(partial_ref[w], partial_ref[w + 1])

    own_ref[0] = partial_ref[0, :half, :half].astype(BF16)
    own_ref[1] = partial_ref[0, :half, half:].astype(BF16)
    own_ref[2] = partial_ref[0, half:, half:].astype(BF16)


def fold_kernel(position_ref, products_ref, partial_ref, out_ref, whole, later):
    count = products_ref.shape[0]
    windows, members, _ = partial_ref.shape
    half = members // 2
    position = position_ref[0]
    whole[...] = jnp.zeros_like(whole)
    later[...] = (
        lax.broadcasted_iota(jnp.int32, (members, members), 0)
        == lax.broadcasted_iota(jnp.int32, (members, members), 1)
    ).astype(F32)

    @pl.loop(0, count - 1 - position)
    def _(turn):
        source = count - 1 - turn
        whole[:half, :half] = products_ref[source, 0]
        whole[:half, half:] = products_ref[source, 1]
        whole[half:, half:] = products_ref[source, 2]
        high, low = halves(later[...])
        left = whole[...]
        later[...] = dot_any(left, high, ((1,), (0,))) + dot_any(left, low, ((1,), (0,)))

    @pl.loop(0, windows)
    def _(w):
        out_ref[w] = dot_three(partial_ref[w], later[...]).astype(BF16)


def local(anomalies, obs_cells, obs_counts, obs_precision, inflation):
    windows, _, cell_width, members = anomalies.shape
    half = members // 2
    slots = obs_cells.shape[1]
    first_cell = lax.axis_index("cell") * cell_width
    offsets = obs_cells - first_cell
    picked = jax.vmap(lambda field, where_at: field[0][where_at])(anomalies, offsets)
    live = jnp.arange(slots, dtype=jnp.int32)[None, :] < obs_counts
    weights = jnp.where(live, obs_precision, jnp.float32(0.0))
    gathered = lax.all_gather(picked, "cell", axis=1, tiled=True)
    gathered_weights = lax.all_gather(weights, "cell", axis=1, tiled=True)
    vmem = pl.BlockSpec(memory_space=pltpu.VMEM)
    smem = pl.BlockSpec(memory_space=pltpu.SMEM)
    partial, own = pl.pallas_call(
        transforms_kernel,
        out_shape=(
            jax.ShapeDtypeStruct((windows, members, members), F32),
            jax.ShapeDtypeStruct((3, half, half), BF16),
        ),
        in_specs=[smem, vmem, vmem],
        out_specs=(vmem, vmem),
        scratch_shapes=[pltpu.VMEM((windows, members, members), F32)]
        + [pltpu.VMEM((windows, half, half), F32)] * 4,
        name="transforms",
    )(inflation, gathered, gathered_weights[:, :, None])
    products = lax.all_gather(own, "tm", axis=0)
    weight_mats = pl.pallas_call(
        fold_kernel,
        out_shape=jax.ShapeDtypeStruct((windows, members, members), BF16),
        in_specs=[smem, vmem, vmem],
        out_specs=vmem,
        scratch_shapes=[pltpu.VMEM((members, members), BF16), pltpu.VMEM((members, members), F32)],
        name="fold",
    )(lax.axis_index("tm").astype(jnp.int32)[None], products, partial)
    flat = anomalies.reshape(windows, 2 * cell_width, members)
    result = jnp.einsum("wcm,wmn->wcn", flat, weight_mats, preferred_element_type=jnp.float32)
    return result.astype(jnp.bfloat16).reshape(anomalies.shape)


def solution(mesh):
    placed = (
        P("tm", None, "cell", None),
        P("tm", "cell"),
        P("tm", "cell"),
        P("tm", "cell"),
        P("tm"),
    )
    return jax.shard_map(
        local, mesh=mesh, in_specs=placed, out_specs=P("tm", None, "cell", None), check_vma=False
    )
```

```python
import jax
import jax.numpy as jnp
from jax import lax
from jax.experimental import pallas as pl
from jax.experimental.pallas import tpu as pltpu
from jax.sharding import PartitionSpec as P

F32 = jnp.float32
BF16 = jnp.bfloat16


def dot_any(left, right, dims):
    return lax.dot_general(left, right, (dims, ((), ())), preferred_element_type=F32)


def halves(value):
    high = value.astype(BF16)
    return high, (value - high.astype(F32)).astype(BF16)


def dot_three(left, right, dims=((1,), (0,))):
    lh, ll = halves(left)
    rh, rl = halves(right)
    return dot_any(lh, rh, dims) + (dot_any(lh, rl, dims) + dot_any(ll, rh, dims))


def dot_full(left, right, dims=((1,), (0,))):
    return lax.dot_general(
        left, right, (dims, ((), ())), precision=lax.Precision.HIGHEST, preferred_element_type=F32
    )


def eliminate(matrices):
    size = matrices[0].shape[0]
    groups = size // 8
    lane = lax.broadcasted_iota(jnp.int32, (8, size), 1)
    sub = lax.broadcasted_iota(jnp.int32, (8, size), 0)
    work = [[m[8 * g : 8 * g + 8, :] for g in range(groups)] for m in matrices]
    for k in range(0, size, 2):
        g, r = divmod(k, 8)
        first_lane, second_lane = lane == k, lane == k + 1
        either = first_lane | second_lane
        for rows in work:
            own = rows[g]
            near = jnp.broadcast_to(own[:, k : k + 1], (8, size))
            far = jnp.broadcast_to(own[:, k + 1 : k + 2], (8, size))
            d0 = jnp.broadcast_to(near[r : r + 1, :], (8, size))
            m = jnp.broadcast_to(near[r + 1 : r + 2, :], (8, size))
            e = jnp.broadcast_to(far[r + 1 : r + 2, :], (8, size))
            row0 = jnp.broadcast_to(own[r : r + 1, :], (8, size))
            row1 = jnp.broadcast_to(own[r + 1 : r + 2, :], (8, size))
            i0 = 1.0 / d0
            step = m * i0
            i1 = 1.0 / (e - step * m)
            row0_one = jnp.where(first_lane, 1.0, row0)
            row1_mid = jnp.where(first_lane, 0.0, row1) - step * row0_one
            p0 = jnp.where(second_lane, 0.0, row0_one) * i0
            p1 = jnp.where(second_lane, 1.0, row1_mid) * i1
            for i in range(g, groups):
                if i == g:
                    c0, c1 = near, far
                else:
                    c0 = jnp.broadcast_to(rows[i][:, k : k + 1], (8, size))
                    c1 = jnp.broadcast_to(rows[i][:, k + 1 : k + 2], (8, size))
                c1 = c1 - c0 * step
                new = jnp.where(either, 0.0, rows[i]) - c0 * p0 - c1 * p1
                if i == g:
                    new = jnp.where(sub <= r, own, jnp.where(sub == r + 1, row1_mid, new))
                rows[i] = new
    results = []
    for rows in work:
        pieces = []
        for g in range(groups):
            row = sub + 8 * g
            pivot = jnp.sum(jnp.where(lane == row, rows[g], 0.0), axis=1, keepdims=True)
            unit = jnp.where(lane < row, rows[g], jnp.where(lane == row, 1.0, 0.0))
            pieces.append(unit * lax.rsqrt(pivot))
        results.append(jnp.concatenate(pieces, axis=0))
    return results


def transforms_kernel(
    rho_ref, picked_ref, weight_ref, partial_ref, own_ref, gram, first_inv, second_inv, low_ref, mid_ref
):
    blocks, windows, slots, members = picked_ref.shape
    half = members // 2
    slot_eye = (
        lax.broadcasted_iota(jnp.int32, (slots, slots), 0)
        == lax.broadcasted_iota(jnp.int32, (slots, slots), 1)
    )
    eye = (
        lax.broadcasted_iota(jnp.int32, (members, members), 0)
        == lax.broadcasted_iota(jnp.int32, (members, members), 1)
    )
    tn = ((0,), (0,))
    nt = ((1,), (1,))

    @pl.loop(0, windows)
    def _(w):
        rows = jnp.concatenate([picked_ref[n, w] for n in range(blocks)], axis=0)
        columns = [
            jnp.sum(
                jnp.where(slot_eye, weight_ref[n, pl.ds(w, 1), :], 0.0), axis=1, keepdims=True
            )
            for n in range(blocks)
        ]
        high, low = halves(rows.astype(F32) * jnp.concatenate(columns, axis=0))
        total = dot_any(high, rows, tn) + dot_any(low, rows, tn)
        gram[w] = total + jnp.where(eye, F32(members - 1.0), 0.0)

    for w, value in enumerate(eliminate([gram[w, :half, :half] for w in range(windows)])):
        first_inv[w] = value

    @pl.loop(0, windows)
    def _(w):
        lower = dot_full(gram[w, half:, :half], first_inv[w], nt)
        low_ref[w] = lower
        gram[w, half:, half:] -= dot_full(lower, lower, nt)
        mid_ref[w] = dot_full(lower, first_inv[w])

    for w, value in enumerate(eliminate([gram[w, half:, half:] for w in range(windows)])):
        second_inv[w] = value

    zero = jnp.zeros((half, half), F32)

    @pl.loop(0, windows)
    def _(w):
        scale = rho_ref[w] * jnp.sqrt(F32(members - 1.0))
        cross = -dot_full(second_inv[w], mid_ref[w])
        partial_ref[w, :half, :half] = scale * first_inv[w].T
        partial_ref[w, :half, half:] = scale * cross.T
        partial_ref[w, half:, :half] = zero
        partial_ref[w, half:, half:] = scale * second_inv[w].T

    @pl.loop(0, windows - 1)
    def _(turn):
        w = windows - 2 - turn
        partial_ref[w] = dot_three(partial_ref[w], partial_ref[w + 1])

    own_ref[0] = partial_ref[0, :half, :half].astype(BF16)
    own_ref[1] = partial_ref[0, :half, half:].astype(BF16)
    own_ref[2] = partial_ref[0, half:, half:].astype(BF16)


def fold_kernel(position_ref, products_ref, partial_ref, out_ref, whole, later):
    count = products_ref.shape[0]
    windows, members, _ = partial_ref.shape
    half = members // 2
    position = position_ref[0]
    whole[...] = jnp.zeros_like(whole)
    later[...] = (
        lax.broadcasted_iota(jnp.int32, (members, members), 0)
        == lax.broadcasted_iota(jnp.int32, (members, members), 1)
    ).astype(F32)

    @pl.loop(0, count - 1 - position)
    def _(turn):
        source = count - 1 - turn
        whole[:half, :half] = products_ref[source, 0]
        whole[:half, half:] = products_ref[source, 1]
        whole[half:, half:] = products_ref[source, 2]
        high, low = halves(later[...])
        left = whole[...]
        later[...] = dot_any(left, high, ((1,), (0,))) + dot_any(left, low, ((1,), (0,)))

    @pl.loop(0, windows)
    def _(w):
        out_ref[w] = dot_three(partial_ref[w], later[...]).astype(BF16)


def exchange_kernel(axis, count, one_way, items, *refs):
    ins, outs = refs[:items], refs[items : 2 * items]
    send_sem, recv_sem = refs[2 * items :]
    me = lax.axis_index(axis)
    barrier = pltpu.get_barrier_semaphore()
    for shift in range(1, count):
        pl.semaphore_signal(
            barrier,
            inc=1,
            device_id={axis: lax.rem(me + shift, count)},
            device_id_type=pl.DeviceIdType.MESH,
        )
    pl.semaphore_wait(barrier, count - 1)

    def copy_of(shift, item):
        return pltpu.make_async_remote_copy(
            src_ref=ins[item],
            dst_ref=outs[item].at[me],
            send_sem=send_sem.at[item, shift],
            recv_sem=recv_sem.at[item, shift],
            device_id={axis: lax.rem(me + count - shift, count)},
            device_id_type=pl.DeviceIdType.MESH,
        )

    def when(condition, action):
        if one_way:
            pl.when(condition)(action)
        else:
            action()

    order = [(shift, item) for shift in range(1, count) for item in range(items)]
    for shift, item in order:
        when(me >= shift, lambda: copy_of(shift, item).start())
    if not one_way:
        for item in range(items):
            outs[item][me] = ins[item][...]
    for shift, item in order:
        when(me >= shift, lambda: copy_of(shift, item).wait_send())
        when(me + shift < count, lambda: copy_of(shift, item).wait_recv())


def exchange(axis, one_way, collective_id, *values):
    count = lax.axis_size(axis)
    items = len(values)
    vmem = pl.BlockSpec(memory_space=pltpu.VMEM)
    return pl.pallas_call(
        lambda *refs: exchange_kernel(axis, count, one_way, items, *refs),
        out_shape=tuple(jax.ShapeDtypeStruct((count,) + v.shape, v.dtype) for v in values),
        in_specs=[vmem] * items,
        out_specs=(vmem,) * items,
        scratch_shapes=[
            pltpu.SemaphoreType.DMA((items, count)),
            pltpu.SemaphoreType.DMA((items, count)),
        ],
        compiler_params=pltpu.CompilerParams(collective_id=collective_id, has_side_effects=True),
        name="exchange_" + axis,
    )(*values)


def apply_kernel(field_ref, weight_ref, out_ref):
    out_ref[0] = jnp.dot(field_ref[0], weight_ref[0], preferred_element_type=F32).astype(
        out_ref.dtype
    )


def local(anomalies, obs_cells, obs_counts, obs_precision, inflation):
    windows, _, cell_width, members = anomalies.shape
    half = members // 2
    slots = obs_cells.shape[1]
    first_cell = lax.axis_index("cell") * cell_width
    offsets = obs_cells - first_cell
    picked = jax.vmap(lambda field, where_at: field[0][where_at])(anomalies, offsets)
    live = jnp.arange(slots, dtype=jnp.int32)[None, :] < obs_counts
    weights = jnp.where(live, obs_precision, jnp.float32(0.0))
    gathered, gathered_weights = exchange("cell", False, 0, picked, weights)
    vmem = pl.BlockSpec(memory_space=pltpu.VMEM)
    smem = pl.BlockSpec(memory_space=pltpu.SMEM)
    partial, own = pl.pallas_call(
        transforms_kernel,
        out_shape=(
            jax.ShapeDtypeStruct((windows, members, members), F32),
            jax.ShapeDtypeStruct((3, half, half), BF16),
        ),
        in_specs=[smem, vmem, vmem],
        out_specs=(vmem, vmem),
        scratch_shapes=[pltpu.VMEM((windows, members, members), F32)]
        + [pltpu.VMEM((windows, half, half), F32)] * 4,
        name="transforms",
    )(inflation, gathered, gathered_weights)
    (products,) = exchange("tm", True, 1, own)
    weight_mats = pl.pallas_call(
        fold_kernel,
        out_shape=jax.ShapeDtypeStruct((windows, members, members), BF16),
        in_specs=[smem, vmem, vmem],
        out_specs=vmem,
        scratch_shapes=[pltpu.VMEM((members, members), BF16), pltpu.VMEM((members, members), F32)],
        name="fold",
    )(lax.axis_index("tm").astype(jnp.int32)[None], products, partial)
    flat = anomalies.reshape(windows, 2 * cell_width, members)
    tile = min(2048, 2 * cell_width)
    result = pl.pallas_call(
        apply_kernel,
        out_shape=jax.ShapeDtypeStruct(flat.shape, BF16),
        grid=(windows, 2 * cell_width // tile),
        in_specs=[
            pl.BlockSpec((1, tile, members), lambda w, c: (w, c, 0)),
            pl.BlockSpec((1, members, members), lambda w, c: (w, 0, 0)),
        ],
        out_specs=pl.BlockSpec((1, tile, members), lambda w, c: (w, c, 0)),
        name="apply",
    )(flat, weight_mats)
    return result.reshape(anomalies.shape)


def solution(mesh):
    placed = (
        P("tm", None, "cell", None),
        P("tm", "cell"),
        P("tm", "cell"),
        P("tm", "cell"),
        P("tm"),
    )
    return jax.shard_map(
        local, mesh=mesh, in_specs=placed, out_specs=P("tm", None, "cell", None), check_vma=False
    )
```
